32 devices in a mesh: dp: 4 (over y, core), seq: 8 (over z, x).
Axes of the slice: x: 2, y: 2, z: 4, core: 2. Of those that a mesh axis runs over, the one named last changes fastest.
Arguments:
- queries: bfloat16 [32, 2048, 512], P('dp', 'seq'), may hold values from -6 to 6
- enc_keys: bfloat16 [32, 2048, 512], P('dp', 'seq'), may hold values from -6 to 6
- enc_values: bfloat16 [32, 2048, 512], P('dp', 'seq'), may hold values from -6 to 6
- dec_ids: int32 [32, 2048], P('dp', 'seq'), may hold values from 0 to 15, never falling along the last dimension, each value on 1 to 512 neighbouring positions
- enc_ids: int32 [32, 2048], P('dp', 'seq'), may hold values from 0 to 15, never falling along the last dimension, each value on 1 to 512 neighbouring positions
Outputs:
- context: bfloat16 [32, 2048, 512], P('dp', 'seq')
The draws below stay inside these ranges and needn't reach their ends.
Inputs may be any that keep to these rules, and one draw needn't show every extreme that they name: `dec_ids`: along each row the numbers never fall; every number from 0 to 15 occurs in every row; a document holds 1 to 512 positions of a row, and some document holds exactly 512. `enc_ids`: along each row the numbers never fall; every number from 0 to 15 occurs in every row; a document holds 1 to 512 positions of a row, and some document holds exactly 512.
All inputs are finite; a program needn't handle non-finite values.
Results may differ from the reference program's by a relative error of at most 0.0047.
Values may be sent and summed in bfloat16 or wider, within the bound.
No kernel may reach another device: no remote copies, remote signals or barrier semaphores. Data moves between devices by JAX's collectives and lax.ppermute only.
A program may use at most 128 MiB of HBM per device.

```python
import math
import jax
import jax.numpy as jnp
import numpy as np
from jax import lax

HEAD_DIM = 64
LEN = 2048
NDOC = 16
MOST = 512
HEADS = 8
INNER = 512
BATCH = 32


def draw_queries(key, part):
    base = jax.random.truncated_normal(jax.random.fold_in(key, 1), -6.0, 6.0, (BATCH, LEN, HEADS * HEAD_DIM), jnp.float32)
    result = 0.25 * base
    return result.astype(jnp.bfloat16)


def draw_enc_keys(key, part):
    base = jax.random.truncated_normal(jax.random.fold_in(key, 3), -6.0, 6.0, (BATCH, LEN, HEADS * HEAD_DIM), jnp.float32)
    result = base
    return result.astype(jnp.bfloat16)


def levels(rng, dims, cuts, least, top_value):
    level, own = 1.0, jax.random.fold_in(rng, 6)
    for dim, parts in cuts:
        heights = jnp.exp(jax.random.uniform(jax.random.fold_in(own, dim), (parts,), jnp.float32, least / len(cuts), top_value / len(cuts)))
        level = level * jnp.repeat(heights, dims[dim] // parts).reshape([-1 if axis == dim else 1 for axis in range(len(dims))])
    return level


def split_up(amount, total, most, lean):
    weights = [(1 << 20) // math.isqrt(grade ** lean) + 1 for grade in range(2, amount + 1)]
    surplus, given = total - most - (amount - 1), [1] * (amount - 1)
    while surplus > 0:
        free = [i for i in range(amount - 1) if given[i] < most]
        pool, left = sum([weights[i] for i in free]), surplus
        for i in free:
            addition = min(most - given[i], max(1, left * weights[i] // pool), surplus)
            given[i] = given[i] + addition
            surplus = surplus - addition
    return np.array([most] + given)


def uneven_parts(stream_key, number_of, total, most, slope):
    if number_of == 2:
        one = jax.random.randint(stream_key, (), max(1, total - most), min(most, total - 1) + 1)
        return jnp.stack([one, total - one])
    sizes = jnp.asarray(split_up(number_of, total, most, slope), jnp.int32)
    pairs = (number_of - 1) // 2
    giver, sink = sizes[1:1 + 2 * pairs:2], sizes[2:2 + 2 * pairs:2]
    slack = jnp.minimum(giver - 1, most - sink)
    moved = jax.random.randint(jax.random.fold_in(stream_key, 1), (pairs,), 0, 1 << 20) % (slack + 1)
    sizes = sizes.at[1:1 + 2 * pairs:2].set(giver - moved).at[2:2 + 2 * pairs:2].set(sink + moved)
    return sizes[jax.random.permutation(jax.random.fold_in(stream_key, 2), number_of)]


def scatter_about(key, extent, scale, reach, shards=(), kind=jnp.bfloat16):
    factor_of = levels(key, extent, shards, -0.22, 0.18) if shards else 1.0
    values = jax.random.normal(key, extent, jnp.float32) * scale * factor_of
    return jnp.minimum(jnp.maximum(values, -reach), reach).astype(kind)


def setup_inputs(seed: int = 0) -> dict:
    splits = jax.random.split(jax.random.key(seed), 6)
    return {
        "queries": draw_queries(jax.random.fold_in(splits[5], 71), 0),
        "enc_keys": draw_enc_keys(jax.random.fold_in(splits[5], 71), 0),
        "enc_values": scatter_about(splits[2], (BATCH, LEN, INNER), 1.0, 6.0, ((0, 4), (1, 8))),
        "dec_ids": jax.vmap(lambda own: jnp.searchsorted(jnp.cumsum(uneven_parts(own, NDOC, LEN, MOST, 2)), jnp.arange(LEN), side="right"))(jax.random.split(splits[3], BATCH)).reshape((BATCH, LEN)).astype(jnp.int32),
        "enc_ids": jax.vmap(lambda own: jnp.searchsorted(jnp.cumsum(uneven_parts(own, NDOC, LEN, MOST, 2)), jnp.arange(LEN), side="right"))(jax.random.split(splits[4], BATCH)).reshape((BATCH, LEN)).astype(jnp.int32),
    }


masked_score = -1.0e30


def attend_row(query_row, key_row, value_row, dec_row, enc_row):
    query_heads = query_row.astype(jnp.float32).reshape(LEN, HEADS, HEAD_DIM)
    key_heads = key_row.astype(jnp.float32).reshape(LEN, HEADS, HEAD_DIM)
    value_heads = value_row.astype(jnp.float32).reshape(LEN, HEADS, HEAD_DIM)
    query_span = min(512, LEN)
    pieces = []
    for offset in range(0, LEN, query_span):
        scores = jnp.einsum("qhd,khd->hqk", query_heads[offset:offset + query_span], key_heads,
                            precision=lax.Precision.HIGHEST)
        allowed = (dec_row[offset:offset + query_span][:, None] == enc_row[None, :])[None]
        scores = jnp.where(allowed, scores, masked_score)
        row_peak = jnp.max(scores, axis=2, keepdims=True)
        expos = jnp.where(allowed, jnp.exp(scores - row_peak), 0.0)
        row_total = jnp.sum(expos, axis=2, keepdims=True)
        weights = (expos / row_total).astype(jnp.bfloat16)
        weights = lax.optimization_barrier(weights).astype(jnp.float32)
        summed = jnp.einsum("hqk,khd->qhd", weights, value_heads, precision=lax.Precision.HIGHEST)
        pieces.append(summed.reshape(query_span, HEADS * HEAD_DIM).astype(jnp.bfloat16))
    return jnp.concatenate(pieces, axis=0)


def reference(queries, enc_keys, enc_values, dec_ids, enc_ids):
    def one_row(members):
        return attend_row(members[0], members[1], members[2], members[3], members[4])

    return lax.map(one_row, (queries, enc_keys, enc_values, dec_ids, enc_ids))
```

```python
import functools
import jax
import jax.numpy as jnp
from jax import lax
from jax.experimental import pallas as pl
from jax.experimental.pallas import tpu as pltpu
from jax.sharding import Mesh, PartitionSpec as P

HEAD_DIM = 64
NDOC = 16
LANES = 2 * HEAD_DIM
BLOCK = 64
CHUNK = 4
NEG = -1.0e30
CLASSES = ((0.4375, 0.09375, 0.015625), (0.53125, 0.15625, 0.015625), (0.625, 0.1875, 0.03125))
FORCE = None


def halves():
    lane = lax.broadcasted_iota(jnp.int32, (1, LANES), 1)
    low = jnp.where(lane < HEAD_DIM, 1.0, 0.0)
    return low.astype(jnp.bfloat16), (1.0 - low).astype(jnp.bfloat16)


def interleave(a, b):
    first = jnp.concatenate([a[:, :HEAD_DIM], b[:, :HEAD_DIM]], axis=1)
    second = jnp.concatenate([a[:, HEAD_DIM:], b[:, HEAD_DIM:]], axis=1)
    return first, second


def pack_pair_kernel(k_ref, v_ref, out_ref):
    for j in range(k_ref.shape[2] // LANES):
        cols = slice(j * LANES, (j + 1) * LANES)
        first, second = interleave(k_ref[0, :, cols], v_ref[0, :, cols])
        out_ref[2 * j, 0] = first
        out_ref[2 * j + 1, 0] = second


def pack_pair(keys, values):
    rows, span, inner = keys.shape
    heads = inner // HEAD_DIM
    return pl.pallas_call(
        pack_pair_kernel,
        grid=(rows,),
        in_specs=[pl.BlockSpec((1, span, inner), lambda r: (r, 0, 0))] * 2,
        out_specs=pl.BlockSpec((heads, 1, span, LANES), lambda r: (0, r, 0, 0)),
        out_shape=jax.ShapeDtypeStruct((heads, rows, span, LANES), keys.dtype),
        cost_estimate=pl.CostEstimate(
            flops=keys.size * 16, bytes_accessed=keys.size * 8, transcendentals=0
        ),
        name="pack_kv",
    )(keys, values)


def pack_queries_kernel(q_ref, out_ref):
    tile = out_ref.shape[2]
    for j in range(q_ref.shape[2] // LANES):
        cols = slice(j * LANES, (j + 1) * LANES)
        first, second = interleave(q_ref[0, :tile, cols], q_ref[0, tile:, cols])
        out_ref[2 * j, 0] = first
        out_ref[2 * j + 1, 0] = second


def pack_queries(queries):
    rows, span, inner = queries.shape
    heads = inner // HEAD_DIM
    return pl.pallas_call(
        pack_queries_kernel,
        grid=(rows,),
        in_specs=[pl.BlockSpec((1, span, inner), lambda r: (r, 0, 0))],
        out_specs=pl.BlockSpec((heads, 1, span // 2, LANES), lambda r: (0, r, 0, 0)),
        out_shape=jax.ShapeDtypeStruct((heads, rows, span // 2, LANES), queries.dtype),
        cost_estimate=pl.CostEstimate(
            flops=queries.size * 16, bytes_accessed=queries.size * 4, transcendentals=0
        ),
        name="pack_q",
    )(queries)


def unpack_kernel(o_ref, out_ref):
    tile = o_ref.shape[2]
    for j in range(out_ref.shape[2] // LANES):
        cols = slice(j * LANES, (j + 1) * LANES)
        top, bottom = interleave(o_ref[2 * j, 0], o_ref[2 * j + 1, 0])
        out_ref[0, :tile, cols] = top
        out_ref[0, tile:, cols] = bottom


def unpack(outputs):
    heads, rows, tile, _ = outputs.shape
    inner = heads * HEAD_DIM
    return pl.pallas_call(
        unpack_kernel,
        grid=(rows,),
        in_specs=[pl.BlockSpec((heads, 1, tile, LANES), lambda r: (0, r, 0, 0))],
        out_specs=pl.BlockSpec((1, 2 * tile, inner), lambda r: (r, 0, 0)),
        out_shape=jax.ShapeDtypeStruct((rows, 2 * tile, inner), outputs.dtype),
        cost_estimate=pl.CostEstimate(
            flops=outputs.size * 16, bytes_accessed=outputs.size * 4, transcendentals=0
        ),
        name="unpack_o",
    )(outputs)


class Sizes:
    def __init__(self, mesh_shape, batch, length, inner):
        self.heads = inner // HEAD_DIM
        self.dp = mesh_shape["dp"]
        self.x = self.heads // self.dp
        self.z = mesh_shape["seq"] // self.x
        self.rows = batch
        self.own_rows = batch // self.dp
        self.length = length
        self.span = length // (self.x * self.z)
        self.level = length // self.z
        self.tile = self.span // 2
        self.part_blocks = self.span // BLOCK
        self.level_blocks = self.level // BLOCK
        self.shifts = [s for s in range(-(self.z - 1), self.z) if s]


def spans(sz, counts):
    total = counts.sum(axis=(1, 2)).reshape(sz.rows, 2, NDOC)
    before = jnp.arange(NDOC)[:, None] > jnp.arange(NDOC)[None, :]
    start = jnp.where(before, total[:, :, None, :], 0).sum(axis=3)
    end = start + total
    dec_start, enc_start = start[:, 0], start[:, 1]
    dec_end, enc_end = end[:, 0], end[:, 1]
    first = jnp.arange(sz.z * sz.x)[None, :, None] * sz.span
    last = first + sz.span - 1
    holds = lambda at: (dec_start[:, None] <= at) & (at < dec_end[:, None])
    low = jnp.where(holds(first), enc_start[:, None], 0).sum(axis=2) // BLOCK
    high = (jnp.where(holds(last), enc_end[:, None], 0).sum(axis=2) + BLOCK - 1) // BLOCK
    low, high = low.reshape(sz.rows, sz.z, sz.x), high.reshape(sz.rows, sz.z, sz.x)
    return (dec_start, dec_end, enc_start, enc_end), low, high


def tables(sz, docs, low, high):
    me = lax.axis_index("z")
    need_low, need_high = low[:, :, 0], high[:, :, -1]
    level = jnp.arange(sz.z) * sz.level_blocks
    run_low = jnp.maximum(need_low[:, None, :], level[None, :, None])
    run_high = jnp.minimum(need_high[:, None, :], level[None, :, None] + sz.level_blocks)
    count = jnp.maximum(run_high - run_low, 0)
    earlier = jnp.arange(sz.rows)[:, None] > jnp.arange(sz.rows)[None, :]
    offset = jnp.where(earlier[:, :, None, None], count[None], 0).sum(axis=1)
    sums = count.sum(axis=0)
    gap = jnp.arange(sz.z)[None, :] - jnp.arange(sz.z)[:, None]
    worst = [jnp.where(gap == s, sums, 0).max() for s in sz.shifts]

    shifts = jnp.arange(-(sz.z - 1), sz.z)
    here = jnp.arange(sz.z) == me
    into = (gap[None] == shifts[:, None, None]) & here[None, None, :]
    out_of = (gap[None] == shifts[:, None, None]) & here[None, :, None]
    pick = lambda sel, v: jnp.where(sel[None], v[:, None], 0).sum(axis=(2, 3))
    receive = jnp.stack([pick(into, count), pick(into, offset), pick(into, run_low)])
    send = jnp.stack([pick(out_of, count), pick(out_of, offset), pick(out_of, run_low)])
    mine = lambda v: jnp.where(here[None, :, None], v, 0).sum(axis=1)
    unit_low, unit_high = mine(low), mine(high)
    base = unit_low[:, :1]
    units = jnp.concatenate([base, unit_high[:, -1:], unit_low, unit_high], axis=1)

    dec_start, dec_end, enc_start, enc_end = docs
    ahead = jnp.zeros((sz.rows, HEAD_DIM), jnp.int32)
    rest = LANES - HEAD_DIM - NDOC
    open_low = jnp.zeros((sz.rows, rest), jnp.int32)
    open_high = jnp.full((sz.rows, rest), 1 << 30, jnp.int32)
    row_of = lambda v, fill: jnp.concatenate([ahead, v, fill], axis=1)
    lanes = jnp.stack(
        [row_of(enc_start, open_low), row_of(enc_end, open_high),
         row_of(dec_start, open_low), row_of(dec_end, open_high)], axis=1,
    )
    return receive, send, units, lanes, worst


def select_kernel(sz, send_ref, me_ref, kv_ref, *out_refs):
    per = sz.own_rows * sz.part_blocks
    first = me_ref[0] * sz.level_blocks
    shifts = 2 * sz.z - 1
    for out_ref, shift in zip(out_refs, sz.shifts):
        slot = shift + sz.z - 1

        @pl.loop(0, sz.rows)
        def _(row):
            at = row * shifts + slot
            count, offset = send_ref[0, at], send_ref[1, at]
            low = send_ref[2, at] - first
            base = (row // sz.own_rows) * (sz.x * per) + (row % sz.own_rows) * sz.part_blocks

            @pl.loop(0, count)
            def _(i):
                block = low + i
                source = base + (block // sz.part_blocks) * per + block % sz.part_blocks
                out_ref[offset + i] = kv_ref[source]


def select_blocks(sz, caps, send, me, kv):
    size = sum(caps) * BLOCK * LANES * 2
    return pl.pallas_call(
        functools.partial(select_kernel, sz),
        in_specs=[pl.BlockSpec(memory_space=pltpu.SMEM)] * 2
        + [pl.BlockSpec(memory_space=pltpu.VMEM)],
        out_specs=[pl.BlockSpec(memory_space=pltpu.VMEM)] * len(caps),
        out_shape=[jax.ShapeDtypeStruct((cap, BLOCK, LANES), kv.dtype) for cap in caps],
        cost_estimate=pl.CostEstimate(flops=size, bytes_accessed=2 * size, transcendentals=0),
        name="select_blocks",
    )(send, me, kv)


def attend_kernel(sz, group, whole, receive_ref, units_ref, me_ref, lanes_ref, q_ref, kv_ref, *refs):
    sources = len(sz.shifts)
    others, (o_ref, k_scr, v_scr, s_scr, m_scr, a_scr) = refs[:sources], refs[sources:]
    low_mask, high_mask = halves()
    shifts = 2 * sz.z - 1
    per = sz.own_rows * sz.part_blocks
    me = me_ref[0]
    dp, step = pl.program_id(0), pl.program_id(1)
    width = 2 + 2 * sz.x
    first_row = dp * sz.own_rows + step * group
    position = lax.broadcasted_iota(jnp.int32, (BLOCK, LANES), 0)

    def unit(g, x):
        at = (first_row + g) * width
        base = units_ref[at]
        return units_ref[at + 2 + x] - base, units_ref[at + 2 + sz.x + x] - base

    chunks = 1
    for g in range(group):
        for x in range(sz.x):
            begin, end = unit(g, x)
            chunks = jnp.maximum(chunks, (end - begin + CHUNK - 1) // CHUNK)

    for g in range(group):
        row = first_row + g
        base, stop = units_ref[row * width], units_ref[row * width + 1]
        enc_start, enc_end = lanes_ref[0, g, 0:1, :], lanes_ref[0, g, 1:2, :]

        def put(block, kv, g=g, base=base, enc_start=enc_start, enc_end=enc_end):
            at = pl.multiple_of((block - base) * BLOCK, BLOCK)
            where = position + block * BLOCK
            inside = (where >= enc_start) & (where < enc_end)
            mask = jnp.where(inside, 0.0, NEG).astype(jnp.bfloat16) * high_mask
            k_scr[g, pl.ds(at, BLOCK), :] = kv * low_mask + mask
            v_scr[g, pl.ds(at, BLOCK), :] = kv * high_mask + low_mask

        for slot in range(shifts):
            at = row * shifts + slot
            count, offset, low = receive_ref[0, at], receive_ref[1, at], receive_ref[2, at]
            shift = slot - (sz.z - 1)
            in_level = low - (me - shift) * sz.level_blocks

            @pl.loop(0, count)
            def _(i, slot=slot, shift=shift, offset=offset, low=low, in_level=in_level, put=put, g=g):
                block = in_level + i
                part, inner = block // sz.part_blocks, block % sz.part_blocks
                if shift == 0:
                    row_base = dp * (sz.x * per) + (step * group + g) * sz.part_blocks
                    kv = kv_ref[row_base + part * per + inner]
                elif whole:
                    kv = others[sz.shifts.index(shift)][0, part, g, inner]
                else:
                    kv = others[sz.shifts.index(shift)][offset + i]
                put(low + i, kv)

        tail = chunks * CHUNK
        last = 0
        for x in range(sz.x):
            last = jnp.maximum(last, unit(g, x)[0] + tail)

        @pl.loop(stop - base, last)
        def _(i, g=g):
            at = pl.multiple_of(i * BLOCK, BLOCK)
            k_scr[g, pl.ds(at, BLOCK), :] = jnp.broadcast_to(
                (high_mask * NEG).astype(jnp.bfloat16), (BLOCK, LANES)
            )
            v_scr[g, pl.ds(at, BLOCK), :] = jnp.zeros((BLOCK, LANES), jnp.bfloat16)

    pieces = [(g, x, h) for g in range(group) for x in range(sz.x) for h in range(2)]
    q_position = lax.broadcasted_iota(jnp.int32, (sz.tile, LANES), 0)
    asked = []
    for g, x, h in pieces:
        where = q_position + (me * sz.level + x * sz.span + h * sz.tile)
        inside = (where >= lanes_ref[0, g, 2:3, :]) & (where < lanes_ref[0, g, 3:4, :])
        hot = jnp.where(inside, 1.0, 0.0).astype(jnp.bfloat16) * high_mask
        q = q_ref[0, x, g]
        if h:
            q = pltpu.roll(q.astype(jnp.float32), HEAD_DIM, 1).astype(jnp.bfloat16)
        asked.append(q * low_mask + hot)

    for n in range(len(pieces)):
        m_scr[n] = jnp.full((sz.tile, LANES), -3.0e38, jnp.float32)
        a_scr[n] = jnp.zeros((sz.tile, LANES), jnp.float32)
    keys = CHUNK * BLOCK

    def at_chunk(g, x, c):
        return pl.ds(pl.multiple_of((unit(g, x)[0] + c * CHUNK) * BLOCK, BLOCK), keys)

    @pl.loop(0, chunks)
    def _(c):
        for n, (g, x, h) in enumerate(pieces):
            k = k_scr[g, at_chunk(g, x, c), :]
            s = lax.dot_general(
                asked[n], k, (((1,), (1,)), ((), ())), preferred_element_type=jnp.float32
            )
            s_scr[n, c] = s
            peak = m_scr[n]
            for j in range(0, keys, LANES):
                peak = jnp.maximum(peak, s[:, j : j + LANES])
            m_scr[n] = peak

    for n in range(len(pieces)):
        peak = jnp.max(m_scr[n], axis=1, keepdims=True)
        m_scr[n] = jnp.broadcast_to(peak, (sz.tile, LANES))

    @pl.loop(0, chunks)
    def _(c):
        for n, (g, x, h) in enumerate(pieces):
            peak = m_scr[n]
            s = s_scr[n, c]
            p = jnp.concatenate(
                [jnp.exp(s[:, j : j + LANES] - peak) for j in range(0, keys, LANES)], axis=1
            ).astype(jnp.bfloat16)
            v = v_scr[g, at_chunk(g, x, c), :]
            a_scr[n] += jnp.dot(p, v, preferred_element_type=jnp.float32)

    lane = lax.broadcasted_iota(jnp.int32, (sz.tile, LANES), 1)
    for n in range(0, len(pieces), 2):
        g, x, _ = pieces[n]
        first, second = a_scr[n], a_scr[n + 1]
        top = jnp.where(lane < HEAD_DIM, pltpu.roll(first, HEAD_DIM, 1), second)
        bottom = jnp.where(lane < HEAD_DIM, first, pltpu.roll(second, HEAD_DIM, 1))
        o_ref[0, x, g] = (top / bottom).astype(o_ref.dtype)


def attend(sz, whole, receive, units, me, lanes, q, kv, others):
    group = 2
    tile, blocks = sz.tile, sz.length // BLOCK
    room = 2 * blocks + CHUNK
    pieces = group * sz.x * 2
    lanes = lanes.reshape(sz.dp, sz.own_rows, 4, LANES)
    kv_spec = pl.BlockSpec(memory_space=pltpu.VMEM)
    if whole:
        other_spec = pl.BlockSpec(
            (1, sz.x, group, sz.part_blocks, BLOCK, LANES), lambda d, r, *_: (d, 0, r, 0, 0, 0)
        )
        others = [
            o.reshape(sz.dp, sz.x, sz.own_rows, sz.part_blocks, BLOCK, LANES) for o in others
        ]
    else:
        other_spec = kv_spec
    io_spec = pl.BlockSpec((1, sz.x, group, tile, LANES), lambda d, r, *_: (d, 0, r, 0, 0))
    most = -(-blocks // CHUNK)
    return pl.pallas_call(
        functools.partial(attend_kernel, sz, group, whole),
        grid_spec=pltpu.PrefetchScalarGridSpec(
            num_scalar_prefetch=3,
            grid=(sz.dp, sz.own_rows // group),
            in_specs=[
                pl.BlockSpec((1, group, 4, LANES), lambda d, r, *_: (d, r, 0, 0)),
                io_spec,
                kv_spec,
            ]
            + [other_spec] * len(others),
            out_specs=io_spec,
            scratch_shapes=[
                pltpu.VMEM((group, room * BLOCK, LANES), jnp.bfloat16),
                pltpu.VMEM((group, room * BLOCK, LANES), jnp.bfloat16),
                pltpu.VMEM((pieces, most, tile, CHUNK * BLOCK), jnp.float32),
                pltpu.VMEM((pieces, tile, LANES), jnp.float32),
                pltpu.VMEM((pieces, tile, LANES), jnp.float32),
            ],
        ),
        out_shape=jax.ShapeDtypeStruct((sz.dp, sz.x, sz.own_rows, tile, LANES), q.dtype),
        cost_estimate=pl.CostEstimate(
            flops=sz.rows * sz.level * 512 * 512,
            bytes_accessed=4 * q.size + 4 * kv.size,
            transcendentals=sz.rows * sz.level * 512,
        ),
        name="attend",
    )(receive, units, me, lanes, q, kv, *others)


def local(sz, queries, enc_keys, enc_values, dec_ids, enc_ids):
    plane = ("dp", "x")
    devices = sz.dp * sz.z * sz.x
    numbers = jnp.stack([dec_ids, enc_ids], axis=1)
    counts = (numbers[..., None] == jnp.arange(NDOC)).astype(jnp.int32).sum(axis=2)
    counts = counts.reshape(sz.own_rows, 2 * NDOC)
    counts = lax.all_to_all(
        jnp.broadcast_to(counts[None], (devices,) + counts.shape),
        ("dp", "z", "x"), split_axis=0, concat_axis=0, tiled=True,
    ).reshape(sz.dp, sz.z, sz.x, sz.own_rows, 2 * NDOC)
    docs, low, high = spans(sz, counts)
    receive, send, units, lanes, worst = tables(sz, docs, low, high)
    me = lax.axis_index("z").reshape(1).astype(jnp.int32)
    flat = lambda v: v.reshape(3, -1)

    blocks = sz.rows * sz.level_blocks
    classes = []
    for shares in CLASSES:
        classes.append([int(blocks * shares[min(abs(s), len(shares)) - 1]) for s in sz.shifts])
    index = sum(
        (~functools.reduce(lambda a, b: a & b, [w <= c for w, c in zip(worst, caps)])).astype(jnp.int32)
        for caps in classes
    )
    if FORCE is not None:
        index = jnp.int32(FORCE)

    kv_packed = pack_pair(enc_keys, enc_values)
    q_packed = pack_queries(queries)

    def run(caps, args):
        kv_packed, q_packed, receive, send, units, lanes, me = args
        kv = lax.all_to_all(kv_packed, plane, split_axis=0, concat_axis=0, tiled=True)
        kv = kv.reshape(-1, BLOCK, LANES)
        if caps is None:
            sent = [kv] * len(sz.shifts)
        else:
            sent = select_blocks(sz, caps, flat(send), me, kv)
        others = []
        for buffer, shift in zip(sent, sz.shifts):
            pairs = [(i, i + shift) for i in range(sz.z) if 0 <= i + shift < sz.z]
            others.append(lax.ppermute(buffer, "z", pairs))
        q = lax.all_to_all(q_packed, plane, split_axis=0, concat_axis=0, tiled=True)
        q = q.reshape(sz.dp, sz.x, sz.own_rows, sz.tile, LANES)
        out = attend(
            sz, caps is None, flat(receive), units.reshape(-1), me, lanes, q, kv, others
        )
        out = out.reshape(sz.dp * sz.x, sz.own_rows, sz.tile, LANES)
        out = lax.all_to_all(out, plane, split_axis=0, concat_axis=0, tiled=True)
        return unpack(out)

    args = (kv_packed, q_packed, receive, send, units, lanes, me)
    return lax.switch(index, [functools.partial(run, caps) for caps in classes + [None]], args)


def solution(mesh):
    def whole(queries, enc_keys, enc_values, dec_ids, enc_ids):
        batch, length, inner = queries.shape
        sz = Sizes(mesh.shape, batch, length, inner)
        fine = Mesh(mesh.devices.reshape(sz.dp, sz.z, sz.x), ("dp", "z", "x"))
        wide, narrow = P("dp", ("z", "x"), None), P("dp", ("z", "x"))
        return jax.shard_map(
            functools.partial(local, sz), mesh=fine,
            in_specs=(wide, wide, wide, narrow, narrow), out_specs=wide, check_vma=False,
        )(queries, enc_keys, enc_values, dec_ids, enc_ids)

    return whole
```
